16 devices in a mesh: req: 2 (over z), cp: 8 (over y, x, core).
Axes of the slice: x: 2, y: 2, z: 2, core: 2. Of those that a mesh axis runs over, the one named last changes fastest.
Arguments:
- x: bfloat16 [4096, 5120], P(('req', 'cp')), parts along dimension 0
- pos: int32 [4096], P(('req', 'cp')), parts along dimension 0
- g1: bfloat16 [2, 5120], replicated
- g2: bfloat16 [2, 5120], replicated
- wq: bfloat16 [2, 5120, 5120], replicated
- wk: bfloat16 [2, 5120, 5120], replicated
- wv: bfloat16 [2, 5120, 5120], replicated
- wo: bfloat16 [2, 5120, 5120], replicated
- w1: bfloat16 [2, 5120, 13696], replicated
- w3: bfloat16 [2, 5120, 13696], replicated
- w2: bfloat16 [2, 13696, 5120], replicated
Outputs:
- output 1: bfloat16 [4096, 5120], P(('req', 'cp')), parts along dimension 0
- output 2: bfloat16 [2, 4096, 40, 128], P(None, 'req', 'cp'), parts along dimension 1
- output 3: bfloat16 [2, 4096, 40, 128], P(None, 'req', 'cp'), parts along dimension 1
There are 2 independent parts. The reference program is written for one: setup_inputs(seed, part) draws one part's arguments, and reference() takes and returns one part's arrays. A program takes and returns all parts, laid end to end along the dimension named above; an argument that names none is the same for every part.
All inputs are finite; a program needn't handle non-finite values.
Results may differ from the reference program's by a relative error of at most 0.0183331.
Values are sent between devices in bfloat16 or wider.
A program may use at most 5 GiB of HBM per device.

```python
import jax
import jax.numpy as jnp
from jax import lax
import numpy as np

D = 5120
HEADS = 40
HEAD = 128
FF = 13696
LAYERS = 2
S_DEV = 256
CP = 8

SEQ = CP * S_DEV
SEG = S_DEV // 2


def _layout():
    rows = [np.arange(c * SEG, (c + 1) * SEG) for i in range(CP) for c in (i, 2 * CP - 1 - i)]
    return np.concatenate(rows).astype(np.int32)


def setup_inputs(seed: int = 0, part: int = 0) -> dict:
    key = jax.random.PRNGKey(seed)
    kx, ko = jax.random.split(jax.random.fold_in(key, part))
    ks = jax.random.split(key, 9)
    hd = HEADS * HEAD

    def w(k, shape, scale):
        return (jax.random.normal(k, shape, jnp.float32) * scale).astype(jnp.bfloat16)

    def gain(k):
        return (1.0 + 0.2 * jax.random.normal(k, (LAYERS, D), jnp.float32)).astype(jnp.bfloat16)

    p0 = jax.random.randint(ko, (), 0, 4096, jnp.int32)
    return {
        "x": jax.random.normal(kx, (SEQ, D), jnp.float32).astype(jnp.bfloat16),
        "pos": p0 + jnp.asarray(_layout()),
        "g1": gain(ks[0]),
        "g2": gain(ks[1]),
        "wq": w(ks[2], (LAYERS, D, hd), 1.7 * D ** -0.5),
        "wk": w(ks[3], (LAYERS, D, hd), 1.7 * D ** -0.5),
        "wv": w(ks[4], (LAYERS, D, hd), D ** -0.5),
        "wo": w(ks[5], (LAYERS, hd, D), hd ** -0.5),
        "w1": w(ks[6], (LAYERS, D, FF), D ** -0.5),
        "w3": w(ks[7], (LAYERS, D, FF), D ** -0.5),
        "w2": w(ks[8], (LAYERS, FF, D), FF ** -0.5),
    }


def _norm(x, g):
    x32 = x.astype(jnp.float32)
    r = lax.rsqrt(jnp.mean(x32 * x32, axis=-1, keepdims=True) + 1e-5)
    return (x32 * r * g.astype(jnp.float32)).astype(jnp.bfloat16)


def _rope(t, pos):
    half = HEAD // 2
    inv = 1.0 / (10000.0 ** (jnp.arange(half, dtype=jnp.float32) * (2.0 / HEAD)))
    ang = pos.astype(jnp.float32)[:, None] * inv[None, :]
    c = jnp.cos(ang)[:, None, :]
    s = jnp.sin(ang)[:, None, :]
    t1, t2 = t[..., :half], t[..., half:]
    return jnp.concatenate([t1 * c - t2 * s, t2 * c + t1 * s], axis=-1)


def _attention(q, k, v, pos):
    nb = SEQ // SEG
    scale = HEAD ** -0.5

    def head(a):
        qh, kh, vh = a

        def blk(b):
            qb, pb = b
            s = jnp.dot(qb, kh.T, preferred_element_type=jnp.float32) * scale
            s = jnp.where(pos[None, :] <= pb[:, None], s, -jnp.inf)
            p = jax.nn.softmax(s, axis=-1).astype(jnp.bfloat16)
            return jnp.dot(p, vh, preferred_element_type=jnp.float32).astype(jnp.bfloat16)

        o = lax.map(blk, (qh.reshape(nb, SEG, HEAD), pos.reshape(nb, SEG)))
        return o.reshape(SEQ, HEAD)

    o = lax.map(head, (q.transpose(1, 0, 2), k.transpose(1, 0, 2), v.transpose(1, 0, 2)))
    return o.transpose(1, 0, 2).reshape(SEQ, HEADS * HEAD)


def reference(x, pos, g1, g2, wq, wk, wv, wo, w1, w3, w2):
    order = jnp.argsort(pos)

    def layer(x, w):
        a1, a2, bq, bk, bv, bo, b1, b3, b2 = w
        h = _norm(x, a1)
        q = _rope(jnp.dot(h, bq, preferred_element_type=jnp.float32).reshape(SEQ, HEADS, HEAD), pos).astype(jnp.bfloat16)
        k = _rope(jnp.dot(h, bk, preferred_element_type=jnp.float32).reshape(SEQ, HEADS, HEAD), pos).astype(jnp.bfloat16)
        v = jnp.dot(h, bv, preferred_element_type=jnp.float32).astype(jnp.bfloat16).reshape(SEQ, HEADS, HEAD)
        o = _attention(q, k, v, pos)
        x = (x.astype(jnp.float32) + jnp.dot(o, bo, preferred_element_type=jnp.float32)).astype(jnp.bfloat16)
        h2 = _norm(x, a2)
        u = (jax.nn.silu(jnp.dot(h2, b1, preferred_element_type=jnp.float32))
             * jnp.dot(h2, b3, preferred_element_type=jnp.float32)).astype(jnp.bfloat16)
        x = (x.astype(jnp.float32) + jnp.dot(u, b2, preferred_element_type=jnp.float32)).astype(jnp.bfloat16)
        return x, (k[order], v[order])

    y, (kc, vc) = lax.scan(layer, x, (g1, g2, wq, wk, wv, wo, w1, w3, w2))
    return y, kc, vc
```

```python
import functools

import jax
import jax.numpy as jnp
from jax import lax
from jax.experimental import pallas as pl
from jax.experimental.pallas import tpu as pltpu
from jax.sharding import PartitionSpec as P

HEAD = 128
F32 = jnp.float32
BF16 = jnp.bfloat16
MESH = pl.DeviceIdType.MESH
ANY = pl.BlockSpec(memory_space=pl.ANY)
VM = pl.BlockSpec(memory_space=pltpu.VMEM)
NCP = 8
VLIM = 62 * 1024 * 1024


def _tables(pos):
    half = HEAD // 2
    inv = 1.0 / (10000.0 ** (jnp.arange(half, dtype=F32) * (2.0 / HEAD)))
    ang = pos.astype(F32)[:, None] * inv
    c, s = jnp.cos(ang), jnp.sin(ang)
    return jnp.concatenate([c, c], axis=-1), jnp.concatenate([-s, s], axis=-1)


def _norm(x, g):
    x32 = x.astype(F32)
    r = lax.rsqrt(jnp.mean(x32 * x32, axis=-1, keepdims=True) + 1e-5)
    return (x32 * r * g.astype(F32)).astype(BF16)


def _me():
    me = lax.axis_index('cp')
    return me, me // 4, (me // 2) % 2, me % 2


def _peer(p):
    _, y, x, c = _me()
    return ((y + p // 4) % 2) * 4 + ((x + (p // 2) % 2) % 2) * 2 + (c + p % 2) % 2


def _greet():
    barrier = pltpu.get_barrier_semaphore()
    for p in range(1, NCP):
        pl.semaphore_signal(barrier, inc=1, device_id={'cp': _peer(p)}, device_id_type=MESH)
    pl.semaphore_wait(barrier, NCP - 1)


def _rows(dev, half, seg):
    return pl.multiple_of((dev + half * (2 * NCP - 1 - 2 * dev)) * seg, seg)


def _qkv_kernel(l, x_hbm, g_ref, c_ref, s_ref, wk, wv, wq, k_out, v_out, q_out,
                x_ref, h_ref, wbuf, obuf, xsem, wsem, send, recv, own):
    me = _me()[0]
    wd = wbuf.shape[2]
    seg = x_ref.shape[0] // 2
    nh = wd // HEAD
    nb = wbuf.shape[0]
    ws, outs = (wk, wv, wq), (k_out, v_out, q_out)

    def wcopy(m, j):
        d = _peer(NCP - 1 - j)
        slot = (m * NCP + j) % nb
        return pltpu.make_async_copy(ws[m].at[l, :, pl.ds(pl.multiple_of(d * wd, wd), wd)],
                                     wbuf.at[slot], wsem.at[slot])

    def tile(m, p, half):
        return (obuf.at[m, p, :, pl.ds(half * seg, seg)],
                outs[m].at[:, pl.ds(_rows(me, half, seg), seg)])

    def remote(m, p, half):
        src, dst = tile(m, p, half)
        return pltpu.make_async_remote_copy(
            src_ref=src, dst_ref=dst, send_sem=send.at[m, p, half], recv_sem=recv.at[m, p, half],
            device_id={'cp': _peer(p)}, device_id_type=MESH)

    def local(m, half):
        src, dst = tile(m, 0, half)
        return pltpu.make_async_copy(src, dst, own.at[m, half])

    xcp = pltpu.make_async_copy(x_hbm, x_ref, xsem)
    xcp.start()
    for j in range(nb - 1):
        wcopy(0, j).start()
    _greet()
    xcp.wait()
    h_ref[...] = _norm(x_ref[...], g_ref[...])

    for m in range(3):
        def step(j, _):
            ahead = nb - 1

            @pl.when(j < NCP - ahead)
            def _():
                wcopy(m, j + ahead).start()
            if m < 2:
                @pl.when(j >= NCP - ahead)
                def _():
                    wcopy(m + 1, j + ahead - NCP).start()
            wcopy(m, j).wait()
            p = NCP - 1 - j
            acc = jnp.dot(h_ref[...], wbuf[(m * NCP + j) % nb], preferred_element_type=F32)
            for h in range(nh):
                t = acc[:, h * HEAD:(h + 1) * HEAD]
                if m != 1:
                    t = t * c_ref[...] + pltpu.roll(t, HEAD // 2, 1) * s_ref[...]
                obuf[m, p, h] = t.astype(BF16)

            @pl.when(p > 0)
            def _():
                for half in range(2):
                    remote(m, p, half).start()

            @pl.when(p == 0)
            def _():
                for half in range(2):
                    local(m, half).start()
            return 0

        lax.fori_loop(0, NCP, step, 0)

    for m in range(3):
        for half in range(2):
            local(m, half).wait()

        def fin(p, _):
            for half in range(2):
                remote(m, p, half).wait()
            return 0

        lax.fori_loop(1, NCP, fin, 0)


def _qkv(x, g, c, s, wk, wv, wq, l):
    rows, d = x.shape
    wd = wq.shape[2] // NCP
    nh, nb = wd // HEAD, 3
    out = jax.ShapeDtypeStruct((nh, rows * NCP, HEAD), BF16)
    return pl.pallas_call(
        functools.partial(_qkv_kernel, l),
        in_specs=[ANY, VM, VM, VM, ANY, ANY, ANY],
        out_specs=[ANY] * 3,
        out_shape=[out] * 3,
        scratch_shapes=[
            pltpu.VMEM((rows, d), BF16), pltpu.VMEM((rows, d), BF16),
            pltpu.VMEM((nb, d, wd), BF16), pltpu.VMEM((3, NCP, nh, rows, HEAD), BF16),
            pltpu.SemaphoreType.DMA, pltpu.SemaphoreType.DMA((nb,)),
            pltpu.SemaphoreType.DMA((3, NCP, 2)), pltpu.SemaphoreType.DMA((3, NCP, 2)),
            pltpu.SemaphoreType.DMA((3, 2)),
        ],
        compiler_params=pltpu.CompilerParams(
            vmem_limit_bytes=VLIM, collective_id=2 * l, has_side_effects=True),
        name=f'qkv{l}',
    )(x, g, c, s, wk, wv, wq)


def _attn_kernel(q_ref, k_ref, v_ref, o_out, obuf, acc_ref, send, recv, own):
    me = _me()[0]
    n, bq, wd = obuf.shape
    nh = wd // HEAD
    seg = o_out.shape[0] // 2
    per = bq // seg
    nseg = n * per
    cexp = HEAD ** -0.5 * 1.4426950408889634
    dmask = (lax.broadcasted_iota(jnp.int32, (bq, bq), 0)
             <= lax.broadcasted_iota(jnp.int32, (bq, bq), 1))

    def half_of(sg):
        return sg // NCP

    def owner(sg):
        return sg + half_of(sg) * (2 * NCP - 1 - 2 * sg)

    def place(dev, half):
        return o_out.at[pl.ds(pl.multiple_of(half * seg, seg), seg),
                        pl.ds(pl.multiple_of(dev * wd, wd), wd)]

    def remote(sg):
        return pltpu.make_async_remote_copy(
            src_ref=obuf.at[sg // per, pl.ds(pl.multiple_of((sg % per) * seg, seg), seg)],
            dst_ref=place(me, half_of(sg)),
            send_sem=send.at[sg], recv_sem=recv.at[me, half_of(sg)],
            device_id={'cp': owner(sg)}, device_id_type=MESH)

    def local(sg):
        return pltpu.make_async_copy(
            obuf.at[sg // per, pl.ds(pl.multiple_of((sg % per) * seg, seg), seg)],
            place(me, half_of(sg)), own.at[half_of(sg)])

    _greet()

    def qblock(qi, _):
        qrows = pl.ds(pl.multiple_of(qi * bq, bq), bq)
        acc_ref[...] = jnp.zeros_like(acc_ref)

        def block(kb, carry, diag):
            rows = pl.ds(pl.multiple_of(kb * bq, bq), bq)
            new = []
            for h in range(nh):
                m, den = carry[h]
                sc = lax.dot_general(k_ref[h, rows], q_ref[h, qrows], (((1,), (1,)), ((), ())),
                                     preferred_element_type=F32)
                if diag:
                    sc = jnp.where(dmask, sc, -jnp.inf)
                mn = jnp.maximum(m, jnp.max(sc, axis=0, keepdims=True))
                p = jnp.exp2((sc - mn) * cexp)
                al = jnp.exp2((m - mn) * cexp)
                den = den * al + jnp.sum(p, axis=0, keepdims=True)
                pv = lax.dot_general(v_ref[h, rows], p.astype(BF16), (((0,), (0,)), ((), ())),
                                     preferred_element_type=F32)
                acc_ref[h] = acc_ref[h] * al + pv
                new.append((mn, den))
            return tuple(new)

        init = tuple((jnp.full((1, bq), -jnp.inf, F32), jnp.zeros((1, bq), F32)) for _ in range(nh))
        carry = block(qi, init, True)
        carry = lax.fori_loop(0, qi, lambda kb, cr: block(kb, cr, False), carry)
        for h in range(nh):
            obuf[qi, :, h * HEAD:(h + 1) * HEAD] = (acc_ref[h] / carry[h][1]).T.astype(BF16)

        def push(i, _):
            sg = qi * per + i

            @pl.when(owner(sg) != me)
            def _():
                remote(sg).start()

            @pl.when(owner(sg) == me)
            def _():
                local(sg).start()
            return 0

        lax.fori_loop(0, per, push, 0)
        return 0

    lax.fori_loop(0, n, qblock, 0)

    def fin_send(sg, _):
        @pl.when(owner(sg) != me)
        def _():
            remote(sg).wait_send()

        @pl.when(owner(sg) == me)
        def _():
            local(sg).wait()
        return 0

    lax.fori_loop(0, nseg, fin_send, 0)

    def fin_recv(p, _):
        src = _peer(p)
        for half in range(2):
            pltpu.make_async_remote_copy(
                src_ref=obuf.at[0, pl.ds(0, seg)], dst_ref=place(src, half),
                send_sem=send.at[0], recv_sem=recv.at[src, half],
                device_id={'cp': src}, device_id_type=MESH).wait_recv()
        return 0

    lax.fori_loop(1, NCP, fin_recv, 0)


def _attn(q, k, v, l):
    nh, n, _ = q.shape
    wd, bq = nh * HEAD, 512
    return pl.pallas_call(
        _attn_kernel,
        in_specs=[VM] * 3,
        out_specs=ANY,
        out_shape=jax.ShapeDtypeStruct((n // NCP, wd * NCP), BF16),
        scratch_shapes=[
            pltpu.VMEM((n // bq, bq, wd), BF16), pltpu.VMEM((nh, HEAD, bq), F32),
            pltpu.SemaphoreType.DMA((2 * NCP,)), pltpu.SemaphoreType.DMA((NCP, 2)),
            pltpu.SemaphoreType.DMA((2,)),
        ],
        compiler_params=pltpu.CompilerParams(
            vmem_limit_bytes=VLIM, collective_id=2 * l + 1, has_side_effects=True),
        name=f'attn{l}',
    )(q, k, v)


def _mlp_kernel(l, o_hbm, x_hbm, g_ref, wo, w1, w3, w2, y_ref,
                o_ref, x_ref, h_ref, u_ref, wbuf, dbuf, asem, wsem, dsem):
    d = x_ref.shape[1]
    ff = u_ref.shape[1]
    tn = wbuf.shape[2] // 2
    nb, nd = wbuf.shape[0], dbuf.shape[0]
    n_o, n_up, n_dn = d // (2 * tn), pl.cdiv(ff, tn), d // tn

    def at(w, off):
        return w.at[l, :, pl.ds(pl.multiple_of(off, HEAD), tn)]

    def up_off(j):
        return jnp.minimum(j * tn, ff - tn)

    def pair(i, a, b):
        s = i % nb
        return (pltpu.make_async_copy(a, wbuf.at[s, :, pl.ds(0, tn)], wsem.at[s, 0]),
                pltpu.make_async_copy(b, wbuf.at[s, :, pl.ds(tn, tn)], wsem.at[s, 1]))

    def o_pair(j):
        return pair(j, at(wo, 2 * j * tn), at(wo, (2 * j + 1) * tn))

    def up_pair(j):
        return pair(n_o + j, at(w1, up_off(j)), at(w3, up_off(j)))

    def dn(j):
        s = j % nd
        return pltpu.make_async_copy(at(w2, j * tn), dbuf.at[s], dsem.at[s])

    def start(ps):
        for c in ps:
            c.start()

    def wait(ps):
        for c in ps:
            c.wait()

    acts = (pltpu.make_async_copy(o_hbm, o_ref, asem.at[0]),
            pltpu.make_async_copy(x_hbm, x_ref, asem.at[1]))
    start(acts)
    ahead = nb - 1
    for j in range(ahead):
        start(o_pair(j))
    wait(acts)

    def o_step(j, _):
        @pl.when(j + ahead < n_o)
        def _():
            start(o_pair(j + ahead))

        @pl.when(j + ahead >= n_o)
        def _():
            start(up_pair(j + ahead - n_o))
        wait(o_pair(j))
        cs = pl.ds(pl.multiple_of(2 * j * tn, tn), 2 * tn)
        x_ref[:, cs] = (x_ref[:, cs].astype(F32)
                        + jnp.dot(o_ref[...], wbuf[j % nb], preferred_element_type=F32)).astype(BF16)
        return 0

    lax.fori_loop(0, n_o, o_step, 0)
    h_ref[...] = _norm(x_ref[...], g_ref[...])

    def up_step(j, _):
        @pl.when(j + ahead < n_up)
        def _():
            start(up_pair(j + ahead))

        @pl.when(j == n_up - 4)
        def _():
            for i in range(nd - 1):
                dn(i).start()
        wait(up_pair(j))
        ab = jnp.dot(h_ref[...], wbuf[(n_o + j) % nb], preferred_element_type=F32)
        a, b = ab[:, :tn], ab[:, tn:]
        u_ref[:, pl.ds(pl.multiple_of(up_off(j), HEAD), tn)] = (jax.nn.silu(a) * b).astype(BF16)
        return 0

    lax.fori_loop(0, n_up, up_step, 0)

    def dn_step(j, _):
        @pl.when(j + nd - 1 < n_dn)
        def _():
            dn(j + nd - 1).start()
        dn(j).wait()
        cs = pl.ds(pl.multiple_of(j * tn, tn), tn)
        y_ref[:, cs] = (x_ref[:, cs].astype(F32)
                        + jnp.dot(u_ref[...], dbuf[j % nd], preferred_element_type=F32)).astype(BF16)
        return 0

    lax.fori_loop(0, n_dn, dn_step, 0)


def _mlp(o, x, g, wo, w1, w3, w2, l):
    rows, d = x.shape
    ff = w1.shape[2]
    tn, nb, nd = 256, 3, 3
    return pl.pallas_call(
        functools.partial(_mlp_kernel, l),
        in_specs=[ANY, ANY, VM, ANY, ANY, ANY, ANY],
        out_specs=VM,
        out_shape=jax.ShapeDtypeStruct((rows, d), BF16),
        scratch_shapes=[
            pltpu.VMEM((rows, d), BF16), pltpu.VMEM((rows, d), BF16), pltpu.VMEM((rows, d), BF16),
            pltpu.VMEM((rows, ff), BF16), pltpu.VMEM((nb, d, 2 * tn), BF16), pltpu.VMEM((nd, ff, tn), BF16),
            pltpu.SemaphoreType.DMA((2,)), pltpu.SemaphoreType.DMA((nb, 2)), pltpu.SemaphoreType.DMA((nd,)),
        ],
        compiler_params=pltpu.CompilerParams(vmem_limit_bytes=VLIM),
        name=f'mlp{l}',
    )(o, x, g, wo, w1, w3, w2)


def solution(mesh):
    act = P(('req', 'cp'), None)
    cache = P(None, 'req', 'cp', None)

    def body(x, pos, g1, g2, wq, wk, wv, wo, w1, w3, w2):
        c, s = _tables(pos)
        ks, vs = [], []
        for l in range(wq.shape[0]):
            k, v, q = _qkv(x, g1[l:l + 1], c, s, wk, wv, wq, l)
            o = _attn(q, k, v, l)
            x = _mlp(o, x, g2[l:l + 1], wo, w1, w3, w2, l)
            ks.append(k)
            vs.append(v)
        return x, jnp.stack(ks).transpose(0, 2, 1, 3), jnp.stack(vs).transpose(0, 2, 1, 3)

    return jax.shard_map(body, mesh=mesh, in_specs=(act, P(('req', 'cp'))) + (P(),) * 9,
                         out_specs=(act, cache, cache), check_vma=False)
```

```python
import functools

import jax
import jax.numpy as jnp
from jax import lax
from jax.experimental import pallas as pl
from jax.experimental.pallas import tpu as pltpu
from jax.sharding import PartitionSpec as P

HEAD = 128
F32 = jnp.float32
BF16 = jnp.bfloat16
MESH = pl.DeviceIdType.MESH
ANY = pl.BlockSpec(memory_space=pl.ANY)
VM = pl.BlockSpec(memory_space=pltpu.VMEM)
NCP = 8
BQ = 512
VLIM = 62 * 1024 * 1024


def _tables(pos):
    half = HEAD // 2
    inv = 1.0 / (10000.0 ** (jnp.arange(half, dtype=F32) * (2.0 / HEAD)))
    ang = pos.astype(F32)[:, None] * inv
    c, s = jnp.cos(ang), jnp.sin(ang)
    return jnp.concatenate([c, c], axis=-1), jnp.concatenate([-s, s], axis=-1)


def _norm(x, g):
    x32 = x.astype(F32)
    r = lax.rsqrt(jnp.mean(x32 * x32, axis=-1, keepdims=True) + 1e-5)
    return (x32 * r * g.astype(F32)).astype(BF16)


def _peer(p):
    me = lax.axis_index('cp')
    y, x, c = me // 4, (me // 2) % 2, me % 2
    return ((y + p // 4) % 2) * 4 + ((x + (p // 2) % 2) % 2) * 2 + (c + p % 2) % 2


def _aligned(i, n):
    return pl.multiple_of(i * n, n)


def _layer_kernel(l, groups, x_hbm, g1_ref, g2_ref, c_ref, s_ref, wk, wv, wq, wo, w1, w3, w2,
                  y_out, k_out, v_out,
                  x_ref, h_ref, u_ref, o_ref, wbuf, pbuf, qkv, obuf, acc_ref,
                  asem, wsem, psend, precv, pown, osend, orecv, oown, csem):
    me = lax.axis_index('cp')
    rows, d = x_ref.shape
    ff = u_ref.shape[1]
    seg = rows // 2
    nb = wbuf.shape[0]
    ahead = nb - 1
    wd = d // NCP
    ng = len(groups)
    nqb, bq, _ = obuf.shape
    per = bq // seg
    nseg = nqb * per
    mats = (wk, wv, wq)
    n_p = 3 * NCP
    tn = 512
    n_o, n_up, n_dn = d // tn, pl.cdiv(ff, tn // 2), d // tn
    kcs = [(k, min(d, ff - k)) for k in range(0, ff, d)]
    nk = len(kcs)


    def chunk(src, t, nrow, off, wide, part):
        slot = t % nb
        return pltpu.make_async_copy(
            src, wbuf.at[slot, pl.ds(0, nrow), pl.ds(off, wide)], wsem.at[slot, part])

    def p_chunk(gi, mat, i):
        h0, nh = groups[gi]
        p = NCP - 1 - i % NCP
        col = pl.multiple_of(_peer(p) * wd + h0 * HEAD, HEAD)
        return chunk(mat.at[l, :, pl.ds(col, nh * HEAD)], gi * n_p + i, d, 0, nh * HEAD, 0)

    def p_start(gi, i):
        for m in range(3):
            @pl.when(i // NCP == m)
            def _():
                p_chunk(gi, mats[m], i).start()

    def p_wait(gi, i):
        p_chunk(gi, mats[0], i).wait()

    t_o, t_up = ng * n_p, ng * n_p + n_o
    t_dn = t_up + n_up

    def o_chunks(j):
        return (chunk(wo.at[l, :, pl.ds(_aligned(j, tn), tn)], t_o + j, d, 0, tn, 0),)

    def up_off(j):
        return pl.multiple_of(jnp.minimum(j * (tn // 2), ff - tn // 2), HEAD)

    def up_chunks(j):
        cs = pl.ds(up_off(j), tn // 2)
        return (chunk(w1.at[l, :, cs], t_up + j, d, 0, tn // 2, 0),
                chunk(w3.at[l, :, cs], t_up + j, d, tn // 2, tn // 2, 1))

    def dn_chunks(j, kc):
        k0, kn = kcs[kc]
        return (chunk(w2.at[l, pl.ds(k0, kn), pl.ds(_aligned(j, tn), tn)],
                      t_dn + nk * j + kc, kn, 0, tn, 0),)

    def start(cs):
        for c in cs:
            c.start()

    def wait(cs):
        for c in cs:
            c.wait()

    def stream(n, begin, finish, begin_next, fn):
        def step(j, _):
            @pl.when(j + ahead < n)
            def _():
                begin(j + ahead)

            @pl.when(j + ahead >= n)
            def _():
                begin_next(j + ahead - n)
            finish(j)
            fn(j)
            return 0

        lax.fori_loop(0, n, step, 0)


    def p_pair(gi, m, p, half):
        h0, nh = groups[gi]
        dst = pl.multiple_of((me + half * (2 * NCP - 1 - 2 * me)) * seg, seg)
        return (pbuf.at[m, p, pl.ds(h0, nh), pl.ds(half * seg, seg)],
                qkv.at[m, pl.ds(h0, nh), pl.ds(dst, seg)])

    def p_remote(gi, m, p, half):
        src, dst = p_pair(gi, m, p, half)
        return pltpu.make_async_remote_copy(
            src_ref=src, dst_ref=dst, send_sem=psend.at[gi, m, p, half],
            recv_sem=precv.at[gi, m, p, half], device_id={'cp': _peer(p)}, device_id_type=MESH)

    def p_local(gi, m, half):
        src, dst = p_pair(gi, m, 0, half)
        return pltpu.make_async_copy(src, dst, pown.at[gi, m, half])

    def p_step(gi):
        h0, nh = groups[gi]

        def fn(i):
            m, p = i // NCP, NCP - 1 - i % NCP
            acc = jnp.dot(h_ref[...], wbuf[(gi * n_p + i) % nb, :, 0:nh * HEAD],
                          preferred_element_type=F32)
            for h in range(nh):
                t = acc[:, h * HEAD:(h + 1) * HEAD]
                r = t * c_ref[...] + pltpu.roll(t, HEAD // 2, 1) * s_ref[...]
                pbuf[m, p, h0 + h] = jnp.where(m == 1, t, r).astype(BF16)

            @pl.when(p > 0)
            def _():
                for half in range(2):
                    p_remote(gi, m, p, half).start()

            @pl.when(p == 0)
            def _():
                for half in range(2):
                    p_local(gi, m, half).start()

        return fn

    def p_arrive(gi):
        for m in range(3):
            for half in range(2):
                p_local(gi, m, half).wait()

        def fin(i, _):
            for half in range(2):
                p_remote(gi, i // (NCP - 1), 1 + i % (NCP - 1), half).wait_recv()
            return 0

        lax.fori_loop(0, 3 * (NCP - 1), fin, 0)

    def p_sent(gi):
        def fin(i, _):
            for half in range(2):
                p_remote(gi, i // (NCP - 1), 1 + i % (NCP - 1), half).wait_send()
            return 0

        lax.fori_loop(0, 3 * (NCP - 1), fin, 0)

    def caches(gi):
        h0, nh = groups[gi]
        hs = pl.ds(h0, nh)
        return (pltpu.make_async_copy(qkv.at[0, hs], k_out.at[hs], csem.at[gi, 0]),
                pltpu.make_async_copy(qkv.at[1, hs], v_out.at[hs], csem.at[gi, 1]))


    def half_of(sg):
        return sg // NCP

    def owner(sg):
        return sg + half_of(sg) * (2 * NCP - 1 - 2 * sg)

    def place(gi, dev, half):
        h0, nh = groups[gi]
        return o_ref.at[pl.ds(_aligned(half, seg), seg),
                        pl.ds(pl.multiple_of(dev * wd + h0 * HEAD, HEAD), nh * HEAD)]

    def o_src(gi, sg):
        h0, nh = groups[gi]
        return obuf.at[sg // per, pl.ds(_aligned(sg % per, seg), seg), pl.ds(h0 * HEAD, nh * HEAD)]

    def o_remote(gi, sg):
        return pltpu.make_async_remote_copy(
            src_ref=o_src(gi, sg), dst_ref=place(gi, me, half_of(sg)),
            send_sem=osend.at[gi, sg], recv_sem=orecv.at[gi, me, half_of(sg)],
            device_id={'cp': owner(sg)}, device_id_type=MESH)

    def o_local(gi, sg):
        return pltpu.make_async_copy(o_src(gi, sg), place(gi, me, half_of(sg)), oown.at[gi, half_of(sg)])

    def o_each(gi, lo, n, far, near):
        def one(i, _):
            sg = lo + i

            @pl.when(owner(sg) != me)
            def _():
                far(o_remote(gi, sg))

            @pl.when(owner(sg) == me)
            def _():
                near(o_local(gi, sg))
            return 0

        lax.fori_loop(0, n, one, 0)

    def o_arrive(gi):
        def fin(p, _):
            src = _peer(p)
            for half in range(2):
                pltpu.make_async_remote_copy(
                    src_ref=o_src(gi, 0), dst_ref=place(gi, src, half),
                    send_sem=osend.at[gi, 0], recv_sem=orecv.at[gi, src, half],
                    device_id={'cp': src}, device_id_type=MESH).wait_recv()
            return 0

        lax.fori_loop(1, NCP, fin, 0)


    cexp = HEAD ** -0.5 * 1.4426950408889634
    dmask = (lax.broadcasted_iota(jnp.int32, (bq, bq), 0)
             <= lax.broadcasted_iota(jnp.int32, (bq, bq), 1))

    def attention(gi):
        h0, nh = groups[gi]

        def qblock(qi, _):
            qrows = pl.ds(_aligned(qi, bq), bq)
            for i in range(nh):
                acc_ref[i] = jnp.zeros(acc_ref.shape[1:], F32)

            def block(kb, carry, diag):
                krows = pl.ds(_aligned(kb, bq), bq)
                new = []
                for i in range(nh):
                    m, den = carry[i]
                    sc = lax.dot_general(qkv[0, h0 + i, krows], qkv[2, h0 + i, qrows],
                                         (((1,), (1,)), ((), ())), preferred_element_type=F32)
                    if diag:
                        sc = jnp.where(dmask, sc, -jnp.inf)
                    mn = jnp.maximum(m, jnp.max(sc, axis=0, keepdims=True))
                    p = jnp.exp2((sc - mn) * cexp)
                    al = jnp.exp2((m - mn) * cexp)
                    den = den * al + jnp.sum(p, axis=0, keepdims=True)
                    pv = lax.dot_general(qkv[1, h0 + i, krows], p.astype(BF16),
                                         (((0,), (0,)), ((), ())), preferred_element_type=F32)
                    acc_ref[i] = acc_ref[i] * al + pv
                    new.append((mn, den))
                return tuple(new)

            init = tuple((jnp.full((1, bq), -jnp.inf, F32), jnp.zeros((1, bq), F32)) for _ in range(nh))
            carry = block(qi, init, True)
            carry = lax.fori_loop(0, qi, lambda kb, cr: block(kb, cr, False), carry)
            for i in range(nh):
                obuf[qi, :, (h0 + i) * HEAD:(h0 + i + 1) * HEAD] = (acc_ref[i] / carry[i][1]).T.astype(BF16)
            o_each(gi, qi * per, per, lambda c: c.start(), lambda c: c.start())
            return 0

        lax.fori_loop(0, nqb, qblock, 0)


    xcp = pltpu.make_async_copy(x_hbm, x_ref, asem)
    xcp.start()
    for i in range(ahead):
        p_start(0, i)
    barrier = pltpu.get_barrier_semaphore()
    for p in range(1, NCP):
        pl.semaphore_signal(barrier, inc=1, device_id={'cp': _peer(p)}, device_id_type=MESH)
    pl.semaphore_wait(barrier, NCP - 1)
    xcp.wait()
    h_ref[...] = _norm(x_ref[...], g1_ref[l:l + 1])

    for gi in range(ng):
        if gi + 1 < ng:
            begin_next = functools.partial(p_start, gi + 1)
        else:
            def begin_next(j):
                start(o_chunks(j))
        stream(n_p, functools.partial(p_start, gi), functools.partial(p_wait, gi), begin_next, p_step(gi))

    for gi in range(ng):
        p_arrive(gi)
        start(caches(gi))
        attention(gi)
    for gi in range(ng):
        o_each(gi, 0, nseg, lambda c: c.wait_send(), lambda c: c.wait())
        o_arrive(gi)

    def o_step(j):
        cs = pl.ds(_aligned(j, tn), tn)
        x_ref[:, cs] = (x_ref[:, cs].astype(F32)
                        + jnp.dot(o_ref[...], wbuf[(t_o + j) % nb, :, 0:tn],
                                  preferred_element_type=F32)).astype(BF16)

    stream(n_o, lambda j: start(o_chunks(j)), lambda j: wait(o_chunks(j)),
           lambda j: start(up_chunks(j)), o_step)
    h_ref[...] = _norm(x_ref[...], g2_ref[l:l + 1])

    def up_step(j):
        ab = jnp.dot(h_ref[...], wbuf[(t_up + j) % nb, :, 0:tn], preferred_element_type=F32)
        a, b = ab[:, :tn // 2], ab[:, tn // 2:]
        u_ref[:, pl.ds(up_off(j), tn // 2)] = (jax.nn.silu(a) * b).astype(BF16)

    def dn_next(t):
        for i in range(ahead):
            @pl.when(t == i)
            def _():
                start(dn_chunks(i // nk, i % nk))

    stream(n_up, lambda j: start(up_chunks(j)), lambda j: wait(up_chunks(j)), dn_next, up_step)

    def dn_step(j, _):
        cs = pl.ds(_aligned(j, tn), tn)
        acc = x_ref[:, cs].astype(F32)
        for kc, (k0, kn) in enumerate(kcs):
            jn, kcn = j + (kc + ahead) // nk, (kc + ahead) % nk

            @pl.when(jn < n_dn)
            def _():
                start(dn_chunks(jn, kcn))
            wait(dn_chunks(j, kc))
            acc = acc + jnp.dot(u_ref[:, k0:k0 + kn], wbuf[(t_dn + nk * j + kc) % nb, 0:kn, 0:tn],
                                preferred_element_type=F32)
        x_ref[:, cs] = acc.astype(BF16)
        return 0

    lax.fori_loop(0, n_dn, dn_step, 0)
    ycp = pltpu.make_async_copy(x_ref, y_out, asem)
    ycp.start()
    for gi in range(ng):
        p_sent(gi)
        wait(caches(gi))
    ycp.wait()


def _layer(x, g1, g2, c, s, wk, wv, wq, wo, w1, w3, w2, l):
    rows, d = x.shape
    ff = w1.shape[2]
    nh = wq.shape[2] // NCP // HEAD
    n = rows * NCP
    first = (nh + 1) // 2
    groups = ((0, first), (first, nh - first))
    ng, nb = len(groups), 3
    kv = jax.ShapeDtypeStruct((nh, n, HEAD), BF16)
    dma = pltpu.SemaphoreType.DMA
    return pl.pallas_call(
        functools.partial(_layer_kernel, l, groups),
        in_specs=[ANY] + [VM] * 4 + [ANY] * 7,
        out_specs=[ANY] * 3,
        out_shape=[jax.ShapeDtypeStruct((rows, d), BF16), kv, kv],
        scratch_shapes=[
            pltpu.VMEM((rows, d), BF16), pltpu.VMEM((rows, d), BF16), pltpu.VMEM((rows, ff), BF16),
            pltpu.VMEM((rows, d), BF16), pltpu.VMEM((nb, d, 512), BF16),
            pltpu.VMEM((3, NCP, nh, rows, HEAD), BF16), pltpu.VMEM((3, nh, n, HEAD), BF16),
            pltpu.VMEM((n // BQ, BQ, nh * HEAD), BF16), pltpu.VMEM((first, HEAD, BQ), F32),
            dma, dma((nb, 2)), dma((ng, 3, NCP, 2)), dma((ng, 3, NCP, 2)), dma((ng, 3, 2)),
            dma((ng, 2 * NCP)), dma((ng, NCP, 2)), dma((ng, 2)), dma((ng, 2)),
        ],
        compiler_params=pltpu.CompilerParams(
            vmem_limit_bytes=VLIM, collective_id=l, has_side_effects=True),
        name=f'layer{l}',
    )(x, g1, g2, c, s, wk, wv, wq, wo, w1, w3, w2)


def solution(mesh):
    act = P(('req', 'cp'), None)
    cache = P(None, 'req', 'cp', None)

    def body(x, pos, g1, g2, wq, wk, wv, wo, w1, w3, w2):
        c, s = _tables(pos)
        ks, vs = [], []
        for l in range(wq.shape[0]):
            x, k, v = _layer(x, g1, g2, c, s, wk, wv, wq, wo, w1, w3, w2, l)
            ks.append(k)
            vs.append(v)
        return x, jnp.stack(ks).transpose(0, 2, 1, 3), jnp.stack(vs).transpose(0, 2, 1, 3)

    return jax.shard_map(body, mesh=mesh, in_specs=(act, P(('req', 'cp'))) + (P(),) * 9,
                         out_specs=(act, cache, cache), check_vma=False)
```

```python
import functools

import jax
import jax.numpy as jnp
from jax import lax
from jax.experimental import pallas as pl
from jax.experimental.pallas import tpu as pltpu
from jax.sharding import PartitionSpec as P

HEAD = 128
F32 = jnp.float32
BF16 = jnp.bfloat16
MESH = pl.DeviceIdType.MESH
ANY = pl.BlockSpec(memory_space=pl.ANY)
VM = pl.BlockSpec(memory_space=pltpu.VMEM)
NCP = 8
BQ = 512
VLIM = 62 * 1024 * 1024


def _tables(pos):
    half = HEAD // 2
    inv = 1.0 / (10000.0 ** (jnp.arange(half, dtype=F32) * (2.0 / HEAD)))
    ang = pos.astype(F32)[:, None] * inv
    c, s = jnp.cos(ang), jnp.sin(ang)
    return jnp.concatenate([c, c], axis=-1), jnp.concatenate([-s, s], axis=-1)


def _norm(x, g):
    x32 = x.astype(F32)
    r = lax.rsqrt(jnp.mean(x32 * x32, axis=-1, keepdims=True) + 1e-5)
    return (x32 * r * g.astype(F32)).astype(BF16)


def _peer(p):
    me = lax.axis_index('cp')
    y, x, c = me // 4, (me // 2) % 2, me % 2
    return ((y + p // 4) % 2) * 4 + ((x + (p // 2) % 2) % 2) * 2 + (c + p % 2) % 2


def _aligned(i, n):
    return pl.multiple_of(i * n, n)


def _layers_kernel(nl, groups, x_hbm, g1_ref, g2_ref, c_ref, s_ref, wk, wv, wq, wo, w1, w3, w2,
                  y_out, k_out, v_out,
                  x_ref, h_ref, u_ref, o_ref, wbuf, pbuf, qkv, obuf, acc_ref,
                  asem, wsem, psend, precv, pown, osend, orecv, oown, csem, free):
    me = lax.axis_index('cp')
    rows, d = x_ref.shape
    ff = u_ref.shape[1]
    seg = rows // 2
    nb = wbuf.shape[0]
    ahead = nb - 1
    wd = d // NCP
    ng = len(groups)
    nqb, bq, _ = obuf.shape
    per = bq // seg
    nseg = nqb * per
    mats = (wk, wv, wq)
    n_p = 3 * NCP
    tn = 512
    n_o, n_up, n_dn = d // tn, pl.cdiv(ff, tn // 2), d // tn
    kcs = [(k, min(d, ff - k)) for k in range(0, ff, d)]
    nk = len(kcs)


    def chunk(src, t, nrow, off, wide, part):
        slot = t % nb
        return pltpu.make_async_copy(
            src, wbuf.at[slot, pl.ds(0, nrow), pl.ds(off, wide)], wsem.at[slot, part])

    t_layer = ng * n_p + n_o + n_up + n_dn * nk

    def p_chunk(l, gi, mat, i):
        h0, nh = groups[gi]
        p = NCP - 1 - i % NCP
        col = pl.multiple_of(_peer(p) * wd + h0 * HEAD, HEAD)
        return chunk(mat.at[l, :, pl.ds(col, nh * HEAD)], l * t_layer + gi * n_p + i, d, 0, nh * HEAD, 0)

    def p_start(l, gi, i):
        for m in range(3):
            @pl.when(i // NCP == m)
            def _():
                p_chunk(l, gi, mats[m], i).start()

    def p_wait(l, gi, i):
        p_chunk(l, gi, mats[0], i).wait()

    def start(cs):
        for c in cs:
            c.start()

    def wait(cs):
        for c in cs:
            c.wait()

    def stream(n, begin, finish, begin_next, fn):
        def step(j, _):
            @pl.when(j + ahead < n)
            def _():
                begin(j + ahead)

            @pl.when(j + ahead >= n)
            def _():
                begin_next(j + ahead - n)
            finish(j)
            fn(j)
            return 0

        lax.fori_loop(0, n, step, 0)


    def p_pair(gi, m, p, half):
        h0, nh = groups[gi]
        dst = pl.multiple_of((me + half * (2 * NCP - 1 - 2 * me)) * seg, seg)
        return (pbuf.at[m, p, pl.ds(h0, nh), pl.ds(half * seg, seg)],
                qkv.at[m, pl.ds(h0, nh), pl.ds(dst, seg)])

    def p_remote(gi, m, p, half):
        src, dst = p_pair(gi, m, p, half)
        return pltpu.make_async_remote_copy(
            src_ref=src, dst_ref=dst, send_sem=psend.at[gi, m, p, half],
            recv_sem=precv.at[gi, m, p, half], device_id={'cp': _peer(p)}, device_id_type=MESH)

    def p_local(gi, m, half):
        src, dst = p_pair(gi, m, 0, half)
        return pltpu.make_async_copy(src, dst, pown.at[gi, m, half])

    def p_arrive(gi):
        for m in range(3):
            for half in range(2):
                p_local(gi, m, half).wait()

        def fin(i, _):
            for half in range(2):
                p_remote(gi, i // (NCP - 1), 1 + i % (NCP - 1), half).wait_recv()
            return 0

        lax.fori_loop(0, 3 * (NCP - 1), fin, 0)

    def p_sent(gi):
        def fin(i, _):
            for half in range(2):
                p_remote(gi, i // (NCP - 1), 1 + i % (NCP - 1), half).wait_send()
            return 0

        lax.fori_loop(0, 3 * (NCP - 1), fin, 0)


    def half_of(sg):
        return sg // NCP

    def owner(sg):
        return sg + half_of(sg) * (2 * NCP - 1 - 2 * sg)

    def place(gi, dev, half):
        h0, nh = groups[gi]
        return o_ref.at[pl.ds(_aligned(half, seg), seg),
                        pl.ds(pl.multiple_of(dev * wd + h0 * HEAD, HEAD), nh * HEAD)]

    def o_src(gi, sg):
        h0, nh = groups[gi]
        return obuf.at[sg // per, pl.ds(_aligned(sg % per, seg), seg), pl.ds(h0 * HEAD, nh * HEAD)]

    def o_remote(gi, sg):
        return pltpu.make_async_remote_copy(
            src_ref=o_src(gi, sg), dst_ref=place(gi, me, half_of(sg)),
            send_sem=osend.at[gi, sg], recv_sem=orecv.at[gi, me, half_of(sg)],
            device_id={'cp': owner(sg)}, device_id_type=MESH)

    def o_local(gi, sg):
        return pltpu.make_async_copy(o_src(gi, sg), place(gi, me, half_of(sg)), oown.at[gi, half_of(sg)])

    def o_each(gi, lo, n, far, near):
        def one(i, _):
            sg = lo + i

            @pl.when(owner(sg) != me)
            def _():
                far(o_remote(gi, sg))

            @pl.when(owner(sg) == me)
            def _():
                near(o_local(gi, sg))
            return 0

        lax.fori_loop(0, n, one, 0)

    def o_arrive(gi):
        def fin(p, _):
            src = _peer(p)
            for half in range(2):
                pltpu.make_async_remote_copy(
                    src_ref=o_src(gi, 0), dst_ref=place(gi, src, half),
                    send_sem=osend.at[gi, 0], recv_sem=orecv.at[gi, src, half],
                    device_id={'cp': src}, device_id_type=MESH).wait_recv()
            return 0

        lax.fori_loop(1, NCP, fin, 0)


    cexp = HEAD ** -0.5 * 1.4426950408889634
    dmask = (lax.broadcasted_iota(jnp.int32, (bq, bq), 0)
             <= lax.broadcasted_iota(jnp.int32, (bq, bq), 1))

    def attention(gi):
        h0, nh = groups[gi]

        def qblock(qi, _):
            qrows = pl.ds(_aligned(qi, bq), bq)
            for i in range(nh):
                acc_ref[i] = jnp.zeros(acc_ref.shape[1:], F32)

            def block(kb, carry, diag):
                krows = pl.ds(_aligned(kb, bq), bq)
                new = []
                for i in range(nh):
                    m, den = carry[i]
                    sc = lax.dot_general(qkv[0, h0 + i, krows], qkv[2, h0 + i, qrows],
                                         (((1,), (1,)), ((), ())), preferred_element_type=F32)
                    if diag:
                        sc = jnp.where(dmask, sc, -jnp.inf)
                    mn = jnp.maximum(m, jnp.max(sc, axis=0, keepdims=True))
                    p = jnp.exp2((sc - mn) * cexp)
                    al = jnp.exp2((m - mn) * cexp)
                    den = den * al + jnp.sum(p, axis=0, keepdims=True)
                    pv = lax.dot_general(qkv[1, h0 + i, krows], p.astype(BF16),
                                         (((0,), (0,)), ((), ())), preferred_element_type=F32)
                    acc_ref[i] = acc_ref[i] * al + pv
                    new.append((mn, den))
                return tuple(new)

            init = tuple((jnp.full((1, bq), -jnp.inf, F32), jnp.zeros((1, bq), F32)) for _ in range(nh))
            carry = block(qi, init, True)
            carry = lax.fori_loop(0, qi, lambda kb, cr: block(kb, cr, False), carry)
            for i in range(nh):
                obuf[qi, :, (h0 + i) * HEAD:(h0 + i + 1) * HEAD] = (acc_ref[i] / carry[i][1]).T.astype(BF16)
            o_each(gi, qi * per, per, lambda c: c.start(), lambda c: c.start())
            return 0

        lax.fori_loop(0, nqb, qblock, 0)


    xcp = pltpu.make_async_copy(x_hbm, x_ref, asem)
    xcp.start()
    for i in range(ahead):
        p_start(0, 0, i)
    barrier = pltpu.get_barrier_semaphore()
    for p in range(1, NCP):
        pl.semaphore_signal(barrier, inc=1, device_id={'cp': _peer(p)}, device_id_type=MESH)
    pl.semaphore_wait(barrier, NCP - 1)
    xcp.wait()

    def layer(l):
        base = l * t_layer
        t_o = base + ng * n_p
        t_up = t_o + n_o
        t_dn = t_up + n_up

        def o_chunks(j):
            return (chunk(wo.at[l, :, pl.ds(_aligned(j, tn), tn)], t_o + j, d, 0, tn, 0),)

        def up_off(j):
            return pl.multiple_of(jnp.minimum(j * (tn // 2), ff - tn // 2), HEAD)

        def up_chunks(j):
            cs = pl.ds(up_off(j), tn // 2)
            return (chunk(w1.at[l, :, cs], t_up + j, d, 0, tn // 2, 0),
                    chunk(w3.at[l, :, cs], t_up + j, d, tn // 2, tn // 2, 1))

        def dn_chunks(j, kc):
            k0, kn = kcs[kc]
            return (chunk(w2.at[l, pl.ds(k0, kn), pl.ds(_aligned(j, tn), tn)],
                          t_dn + nk * j + kc, kn, 0, tn, 0),)

        def p_step(gi):
            h0, nh = groups[gi]

            def fn(i):
                m, p = i // NCP, NCP - 1 - i % NCP
                acc = jnp.dot(h_ref[...], wbuf[(base + gi * n_p + i) % nb, :, 0:nh * HEAD],
                              preferred_element_type=F32)
                for h in range(nh):
                    t = acc[:, h * HEAD:(h + 1) * HEAD]
                    r = t * c_ref[...] + pltpu.roll(t, HEAD // 2, 1) * s_ref[...]
                    pbuf[m, p, h0 + h] = jnp.where(m == 1, t, r).astype(BF16)

                @pl.when(p > 0)
                def _():
                    for half in range(2):
                        p_remote(gi, m, p, half).start()

                @pl.when(p == 0)
                def _():
                    for half in range(2):
                        p_local(gi, m, half).start()

            return fn

        def caches(gi):
            h0, nh = groups[gi]
            hs = pl.ds(h0, nh)
            return (pltpu.make_async_copy(qkv.at[0, hs], k_out.at[l, hs], csem.at[gi, 0]),
                    pltpu.make_async_copy(qkv.at[1, hs], v_out.at[l, hs], csem.at[gi, 1]))

        h_ref[...] = _norm(x_ref[...], g1_ref[l:l + 1])
        if l > 0:
            pl.semaphore_wait(free, NCP - 1)

        for gi in range(ng):
            if gi + 1 < ng:
                begin_next = functools.partial(p_start, l, gi + 1)
            else:
                def begin_next(j):
                    start(o_chunks(j))
            stream(n_p, functools.partial(p_start, l, gi), functools.partial(p_wait, l, gi), begin_next, p_step(gi))

        for gi in range(ng):
            p_arrive(gi)
            start(caches(gi))
            if gi + 1 == ng:
                for gj in range(ng):
                    wait(caches(gj))
            attention(gi)
        if l + 1 < nl:
            for p in range(1, NCP):
                pl.semaphore_signal(free, inc=1, device_id={'cp': _peer(p)}, device_id_type=MESH)
        for gi in range(ng):
            o_each(gi, 0, nseg, lambda c: c.wait_send(), lambda c: c.wait())
            o_arrive(gi)

        def o_step(j):
            cs = pl.ds(_aligned(j, tn), tn)
            x_ref[:, cs] = (x_ref[:, cs].astype(F32)
                            + jnp.dot(o_ref[...], wbuf[(t_o + j) % nb, :, 0:tn],
                                      preferred_element_type=F32)).astype(BF16)

        stream(n_o, lambda j: start(o_chunks(j)), lambda j: wait(o_chunks(j)),
               lambda j: start(up_chunks(j)), o_step)
        h_ref[...] = _norm(x_ref[...], g2_ref[l:l + 1])

        def up_step(j):
            ab = jnp.dot(h_ref[...], wbuf[(t_up + j) % nb, :, 0:tn], preferred_element_type=F32)
            a, b = ab[:, :tn // 2], ab[:, tn // 2:]
            u_ref[:, pl.ds(up_off(j), tn // 2)] = (jax.nn.silu(a) * b).astype(BF16)

        def dn_next(t):
            for i in range(ahead):
                @pl.when(t == i)
                def _():
                    start(dn_chunks(i // nk, i % nk))

        stream(n_up, lambda j: start(up_chunks(j)), lambda j: wait(up_chunks(j)), dn_next, up_step)

        def dn_step(j, _):
            cs = pl.ds(_aligned(j, tn), tn)
            acc = x_ref[:, cs].astype(F32)
            for kc, (k0, kn) in enumerate(kcs):
                jn, kcn = j + (kc + ahead) // nk, (kc + ahead) % nk

                @pl.when(jn < n_dn)
                def _():
                    start(dn_chunks(jn, kcn))
                if l + 1 < nl:
                    @pl.when(jn >= n_dn)
                    def _():
                        p_start(l + 1, 0, nk * (jn - n_dn) + kcn)
                wait(dn_chunks(j, kc))
                acc = acc + jnp.dot(u_ref[:, k0:k0 + kn], wbuf[(t_dn + nk * j + kc) % nb, 0:kn, 0:tn],
                                    preferred_element_type=F32)
            x_ref[:, cs] = acc.astype(BF16)
            return 0

        lax.fori_loop(0, n_dn, dn_step, 0)
        for gi in range(ng):
            p_sent(gi)

    for l in range(nl):
        layer(l)
    ycp = pltpu.make_async_copy(x_ref, y_out, asem)
    ycp.start()
    ycp.wait()


def _layers(x, g1, g2, c, s, wk, wv, wq, wo, w1, w3, w2):
    rows, d = x.shape
    nl = wq.shape[0]
    ff = w1.shape[2]
    nh = wq.shape[2] // NCP // HEAD
    n = rows * NCP
    first = (nh + 1) // 2
    groups = ((0, first), (first, nh - first))
    ng, nb = len(groups), 4
    kv = jax.ShapeDtypeStruct((nl, nh, n, HEAD), BF16)
    dma = pltpu.SemaphoreType.DMA
    return pl.pallas_call(
        functools.partial(_layers_kernel, nl, groups),
        in_specs=[ANY] + [VM] * 4 + [ANY] * 7,
        out_specs=[ANY] * 3,
        out_shape=[jax.ShapeDtypeStruct((rows, d), BF16), kv, kv],
        scratch_shapes=[
            pltpu.VMEM((rows, d), BF16), pltpu.VMEM((rows, d), BF16), pltpu.VMEM((rows, ff), BF16),
            pltpu.VMEM((rows, d), BF16), pltpu.VMEM((nb, d, 512), BF16),
            pltpu.VMEM((3, NCP, nh, rows, HEAD), BF16), pltpu.VMEM((3, nh, n, HEAD), BF16),
            pltpu.VMEM((n // BQ, BQ, nh * HEAD), BF16), pltpu.VMEM((first, HEAD, BQ), F32),
            dma, dma((nb, 2)), dma((ng, 3, NCP, 2)), dma((ng, 3, NCP, 2)), dma((ng, 3, 2)),
            dma((ng, 2 * NCP)), dma((ng, NCP, 2)), dma((ng, 2)), dma((ng, 2)), pltpu.SemaphoreType.REGULAR,
        ],
        compiler_params=pltpu.CompilerParams(
            vmem_limit_bytes=VLIM, collective_id=0, has_side_effects=True),
        name='layers',
    )(x, g1, g2, c, s, wk, wv, wq, wo, w1, w3, w2)


def solution(mesh):
    act = P(('req', 'cp'), None)
    cache = P(None, 'req', 'cp', None)

    def body(x, pos, g1, g2, wq, wk, wv, wo, w1, w3, w2):
        c, s = _tables(pos)
        x, k, v = _layers(x, g1, g2, c, s, wk, wv, wq, wo, w1, w3, w2)
        return x, k.transpose(0, 2, 1, 3), v.transpose(0, 2, 1, 3)

    return jax.shard_map(body, mesh=mesh, in_specs=(act, P(('req', 'cp'))) + (P(),) * 9,
                         out_specs=(act, cache, cache), check_vma=False)
```
